32 devices in a mesh: grp: 4 (over y, core), brk: 8 (over z, x).
Axes of the slice: x: 2, y: 2, z: 4, core: 2. Of those that a mesh axis runs over, the one named last changes fastest.
Arguments:
- field: float32 [5, 64, 128, 128], P(None, 'brk', 'grp'), may hold values from -6 to 6
- donors: float32 [1024, 640], P(('grp', 'brk')), may hold values from -6 to 6
- donor_block: int32 [4, 8, 8, 128], P('grp', 'brk'), may hold values from 0 to 31
- donor_corner: int32 [4, 8, 8, 128], P('grp', 'brk'), may hold values from 0 to 86, as said below
- donor_weight: float32 [3, 4, 8, 8, 128], P(None, 'grp', 'brk'), may hold values from 0 to 1
- fringe_count: int32 [4, 8, 8], P('grp', 'brk'), may hold values from 64 to 128, as said below
- fringe_cell: int32 [4, 8, 8, 128], P('grp', 'brk'), may hold values from 0 to 32767, as said below
- velocity: float32 [3, 5], replicated, may hold values from -1 to 1
- mixing: float32 [5, 5], replicated, may hold values from -1.5 to 1.5
Outputs:
- advanced: float32 [5, 64, 128, 128], P(None, 'brk', 'grp')
The draws below stay inside these ranges and needn't reach their ends.
Inputs may be any that keep to these rules, and one draw needn't show every extreme that they name: `fringe_cell`: within one brick the receiving cells of all slots are distinct. `fringe_count`: each brick has an owner with exactly 128 live slots, and in each group some owner has 128 live slots from every brick of the group. `donor_corner`: the corner is 32 ox + 8 oy + oz with ox and oy in 0 to 2 and oz in 0 to 6.
All inputs are finite; a program needn't handle non-finite values.
Results may differ from the reference program's by a relative error of at most 0.0003.
Values sent between devices are 32-bit elements; how exact they have to be, the bound alone decides.
A program may use at most 64 MiB of HBM per device.

```python
import jax
import jax.numpy as jnp
from jax import lax

CX = 8
CY = 32
CZ = 128
VARS = 5
BLOCK = 128
BLK_DEV = 32
CAP = 128
NX = 64
NY = 128
BLOCKS = 1024
N_GRP = 4
N_BRK = 8


def draw_donor_corner(key, part):
    keys = jax.random.split(jax.random.fold_in(key, 11), 3)
    shape = (N_GRP, N_BRK, N_BRK, CAP)
    low_x = jax.random.randint(keys[0], shape, 0, 3)
    low_y = jax.random.randint(keys[1], shape, 0, 3)
    low_z = jax.random.randint(keys[2], shape, 0, 7)
    return (low_x * 32 + low_y * 8 + low_z).astype(jnp.int32)


def draw_fringe_count(key, part):
    keys = jax.random.split(jax.random.fold_in(key, 23), 4)
    shape = (N_GRP, N_BRK, N_BRK)
    first = jax.random.randint(keys[0], shape, 1, CAP + 1)
    second = jax.random.randint(keys[1], shape, 1, CAP + 1)
    counts = CAP - first * second // (2 * CAP)
    full_dev = jax.random.randint(keys[2], (N_GRP, N_BRK, 1), 0, N_BRK)
    full_grp = jax.random.randint(keys[3], (N_GRP, 1, 1), 0, N_BRK)
    owner = jnp.arange(N_BRK, dtype=jnp.int32)[None, None, :]
    counts = jnp.where((owner == full_dev) | (owner == full_grp), CAP, counts)
    return counts.astype(jnp.int32)


def draw_fringe_cell(key, part):
    keys = jax.random.split(jax.random.fold_in(key, 37), 2)
    slots = N_BRK * CAP
    stride = CX * CY * CZ // slots
    dev_keys = jax.random.split(keys[0], N_GRP * N_BRK)
    orders = jax.vmap(lambda k: jax.random.permutation(k, slots))(dev_keys)
    jitter = jax.random.randint(keys[1], (N_GRP * N_BRK, slots), 0, stride)
    cells = orders.astype(jnp.int32) * stride + jitter
    return cells.reshape(N_GRP, N_BRK, N_BRK, CAP).astype(jnp.int32)


def set_ends(values, own_key, least, top_value):
    dims = values.shape
    place = [jax.random.randint(jax.random.fold_in(own_key, axis), (), 0, dims[axis]) for axis in range(len(dims))]
    values = values.at[tuple(place)].set(least)
    longest = dims.index(max(dims))
    place[longest] = (place[longest] + 1) % dims[longest]
    return values.at[tuple(place)].set(top_value)


def block_levels(rng, shape, cuts, least, high):
    gain, own = 1.0, jax.random.fold_in(rng, 6)
    for dim, blocks in cuts:
        draws = jnp.exp(jax.random.uniform(jax.random.fold_in(own, dim), (blocks,), jnp.float32, least / len(cuts), high / len(cuts)))
        gain = gain * jnp.repeat(draws, shape[dim] // blocks).reshape([-1 if axis == dim else 1 for axis in range(len(shape))])
    return gain


def normal_values(key, extent, deviation, limit, shards=(), kind=jnp.bfloat16):
    values = jax.random.normal(key, extent, jnp.float32) * deviation
    if len(shards) > 0:
        values = block_levels(key, extent, shards, -0.22, 0.18) * values
    return jnp.clip(values, min=-limit, max=limit).astype(kind)


def setup_inputs(seed: int = 0) -> dict:
    seeds = jax.random.split(jax.random.key(seed), 10)
    return {
        "field": normal_values(seeds[0], (VARS, NX, NY, CZ), 1.0, 6.0, ((1, 8), (2, 4)), jnp.float32),
        "donors": normal_values(seeds[1], (BLOCKS, VARS * BLOCK), 1.0, 6.0, ((0, 32),), jnp.float32),
        "donor_block": set_ends(jax.random.randint(seeds[2], (N_GRP, N_BRK, N_BRK, CAP), 0, BLK_DEV), jax.random.fold_in(seeds[2], 1), 0, BLK_DEV - 1).astype(jnp.int32),
        "donor_corner": draw_donor_corner(jax.random.fold_in(seeds[9], 71), 0),
        "donor_weight": jnp.clip(1.0 * jax.random.uniform(seeds[4], (3, N_GRP, N_BRK, N_BRK, CAP), jnp.float32) ** block_levels(seeds[4], (3, N_GRP, N_BRK, N_BRK, CAP), ((1, 4), (2, 8)), -0.2, 0.2), 0.0, 1.0),
        "fringe_count": draw_fringe_count(jax.random.fold_in(seeds[9], 71), 0),
        "fringe_cell": draw_fringe_cell(jax.random.fold_in(seeds[9], 71), 0),
        "velocity": jnp.clip(jax.random.uniform(seeds[7], (3, VARS), jnp.float32, -1.0, 1.0), -1.0, 1.0),
        "mixing": normal_values(seeds[8], (VARS, VARS), 0.3, 1.5, (), jnp.float32),
    }


time_step = 0.3


def corner_table(corner, weight):
    cell = jnp.arange(128, dtype=jnp.int32)
    cell_x = cell // 32
    cell_y = (cell // 8) % 4
    cell_z = cell % 8
    low_x = (corner // 32)[..., None]
    low_y = ((corner // 8) % 4)[..., None]
    low_z = (corner % 8)[..., None]
    wx = weight[0][..., None]
    wy = weight[1][..., None]
    wz = weight[2][..., None]
    fx = jnp.where(cell_x == low_x, 1.0 - wx, jnp.where(cell_x == low_x + 1, wx, 0.0))
    fy = jnp.where(cell_y == low_y, 1.0 - wy, jnp.where(cell_y == low_y + 1, wy, 0.0))
    fz = jnp.where(cell_z == low_z, 1.0 - wz, jnp.where(cell_z == low_z + 1, wz, 0.0))
    return fx * fy * fz


def upwind(parts):
    plus = (-2.0 * parts[0] + 15.0 * parts[1] - 60.0 * parts[2] + 20.0 * parts[3] + 30.0 * parts[4] - 3.0 * parts[5]) / 60.0
    minus = (3.0 * parts[1] - 30.0 * parts[2] - 20.0 * parts[3] + 60.0 * parts[4] - 15.0 * parts[5] + 2.0 * parts[6]) / 60.0
    return plus, minus


def tendency(padded, velocity, mixing):
    span_x = padded.shape[1] - 6
    span_y = padded.shape[2] - 6
    along_x = [padded[:, k:k + span_x, 3:3 + span_y, :] for k in range(7)]
    along_y = [padded[:, 3:3 + span_x, k:k + span_y, :] for k in range(7)]
    center = along_x[3]
    along_z = [jnp.roll(center, 3 - k, axis=3) for k in range(7)]
    rate = -jnp.einsum("vw,wxyz->vxyz", mixing, center, precision=lax.Precision.HIGHEST)
    for dim, parts in enumerate((along_x, along_y, along_z)):
        speed = velocity[dim][:, None, None, None]
        plus, minus = upwind(parts)
        rate = rate - (jnp.maximum(speed, 0.0) * plus + jnp.minimum(speed, 0.0) * minus)
    return rate


def reference(field, donors, donor_block, donor_corner, donor_weight, fringe_count, fringe_cell, velocity, mixing):
    blocks_all = donors.reshape(N_GRP, N_BRK * BLK_DEV, VARS * BLOCK)

    def per_group(items):
        blocks, blk, corner, weight = items
        index = (jnp.arange(N_BRK, dtype=jnp.int32) * BLK_DEV)[None, :, None] + blk
        rows = blocks[index].reshape(N_BRK, N_BRK, CAP, VARS, BLOCK)
        table = corner_table(corner, weight)
        return jnp.einsum("bocvk,bock->bvoc", rows, table, precision=lax.Precision.HIGHEST)

    values = lax.map(per_group, (blocks_all, donor_block, donor_corner, jnp.transpose(donor_weight, (1, 0, 2, 3, 4))))
    values = jnp.transpose(values, (2, 0, 1, 3, 4))
    group_ids = jnp.arange(N_GRP, dtype=jnp.int32)[:, None, None, None]
    brick_ids = jnp.arange(N_BRK, dtype=jnp.int32)[None, :, None, None]
    slot_ids = jnp.arange(CAP, dtype=jnp.int32)[None, None, None, :]
    live = slot_ids < fringe_count[..., None]
    pos_x = brick_ids * CX + fringe_cell // (CY * CZ)
    pos_y = group_ids * CY + (fringe_cell // CZ) % CY
    pos_z = fringe_cell % CZ
    pos_x = jnp.where(live, pos_x, NX).astype(jnp.int32)
    blended = field.at[:, pos_x, pos_y, pos_z].set(values, mode="drop")
    widths = ((0, 0), (3, 3), (3, 3), (0, 0))
    first = blended + time_step * tendency(jnp.pad(blended, widths, mode="wrap"), velocity, mixing)
    second = first + time_step * tendency(jnp.pad(first, widths, mode="wrap"), velocity, mixing)
    return 0.5 * blended + 0.5 * second
```

```python
import functools

import jax
import jax.numpy as jnp
from jax import lax
from jax.experimental import pallas as pl
from jax.experimental.pallas import tpu as pltpu
from jax.sharding import PartitionSpec as P

time_step = 0.3
PLUS = (-2.0 / 60, 15.0 / 60, -60.0 / 60, 20.0 / 60, 30.0 / 60, -3.0 / 60, 0.0)
MINUS = (0.0, 3.0 / 60, -30.0 / 60, -20.0 / 60, 60.0 / 60, -15.0 / 60, 2.0 / 60)
NT = (((1,), (1,)), ((), ()))


def send(src, dst, sems, index, where):
    copy = pltpu.make_async_remote_copy(
        src_ref=src,
        dst_ref=dst,
        send_sem=sems[0].at[index],
        recv_sem=sems[1].at[index],
        device_id=where,
        device_id_type=pl.DeviceIdType.MESH,
    )
    copy.start()
    return copy


def factors(low, weight, count):
    return [
        jnp.where(low == c, 1.0 - weight, jnp.where(low == c - 1, weight, 0.0))
        for c in range(count)
    ]


def kernel(
    n_grp, n_brk, field_in, donors_in, blk_in, corner_in, weight_in, counts_in, cells_in,
    velocity_in, mixing_in, out, field, donors, blk, corner, weight, counts, cells, velocity,
    mixing, in_sems, req, req_in, res, val_in, cell_out, cell_in, turned, rows_hot, lanes_hot, rows_side,
    lanes_side, u0, y0, u1, y1, faces, ysend, yrecv, coef, send_sems, recv_sems,
):
    loads = [
        pltpu.make_async_copy(src, dst, in_sems.at[i])
        for i, (src, dst) in enumerate(
            (
                (blk_in, blk), (corner_in, corner), (weight_in, weight), (counts_in, counts),
                (cells_in, cells), (velocity_in, velocity), (mixing_in, mixing),
                (donors_in, donors), (field_in, field),
            )
        )
    ]
    for load in loads:
        load.start()
    nvars, cx, cy, cz = field.shape
    nblk = donors.shape[0]
    block = donors.shape[1] // nvars
    sems = (send_sems, recv_sems)
    g = lax.axis_index("grp")
    b = lax.axis_index("brk")
    up_b, down_b = lax.rem(b + 1, n_brk), lax.rem(b + n_brk - 1, n_brk)
    up_g, down_g = lax.rem(g + 1, n_grp), lax.rem(g + n_grp - 1, n_grp)

    barrier = pltpu.get_barrier_semaphore()
    for k in range(1, n_brk):
        pl.semaphore_signal(
            barrier, inc=1, device_id=(g, lax.rem(b + k, n_brk)),
            device_id_type=pl.DeviceIdType.MESH,
        )
    for other in (up_g, down_g):
        pl.semaphore_signal(
            barrier, inc=1, device_id=(other, b), device_id_type=pl.DeviceIdType.MESH
        )

    for load in loads[:-1]:
        load.wait()
    blank = jnp.zeros((3, cz), jnp.float32)
    for o in range(n_brk):
        req[o] = jnp.concatenate(
            [
                blk[o : o + 1].astype(jnp.float32),
                corner[o : o + 1].astype(jnp.float32),
                weight[0, o : o + 1],
                weight[1, o : o + 1],
                weight[2, o : o + 1],
                blank,
            ],
            axis=0,
        )
    req_in[b] = req[b]
    slots = cz
    slot_id = lax.broadcasted_iota(jnp.int32, (1, slots), 1)
    for o in range(n_brk):
        cell_out[o : o + 1] = jnp.where(slot_id < counts[o], cells[o : o + 1], -1)
    for v in range(nvars):
        center = 0.0
        for d in range(3):
            speed = velocity[d, v]
            fast = jnp.maximum(speed, 0.0) * (-time_step)
            slow = jnp.minimum(speed, 0.0) * (-time_step)
            for k in range(7):
                value = fast * PLUS[k] + slow * MINUS[k]
                if k == 3:
                    center = center + value
                else:
                    coef[v, d * 7 + k] = value
        coef[v, 3] = center
        for w in range(nvars):
            coef[v, 21 + w] = mixing[v, w] * (-time_step)

    loads[-1].wait()
    pl.semaphore_wait(barrier, n_brk + 1)
    copies = []
    asks = []
    for k in range(1, n_brk):
        o = lax.rem(b + k, n_brk)
        asks.append(send(req.at[o], req_in.at[b], sems, k, (g, o)))
    base = n_brk
    targets = [
        send(cell_out, cell_in.at[0], sems, base, (g, up_b)),
        send(cell_out, cell_in.at[1], sems, base + 1, (g, down_b)),
    ]
    base = base + 2
    raw = []

    def send_raw(v):
        raw.append(
            send(
                field.at[v, pl.ds(cx - 3, 3)], u0.at[v, pl.ds(0, 3)], sems, base + 2 * v,
                (g, up_b),
            )
        )
        raw.append(
            send(
                field.at[v, pl.ds(0, 3)], u0.at[v, pl.ds(cx + 3, 3)], sems, base + 2 * v + 1,
                (g, down_b),
            )
        )

    for v in range(2):
        send_raw(v)
    value_base = base + 2 * nvars
    exchange_base = value_base + 3 * n_brk

    whole = donors[...]
    first = whole.astype(jnp.bfloat16).astype(jnp.float32)
    second = (whole - first).astype(jnp.bfloat16).astype(jnp.float32)
    third = whole - first - second
    stacked = jnp.concatenate([first, second, third, jnp.zeros_like(whole)], axis=0)
    turned[...] = jnp.transpose(stacked).astype(jnp.bfloat16)

    def mark(targets_ref, top, height, rows_ref, lanes_ref):
        row_id = lax.broadcasted_iota(jnp.int32, (height, slots), 0)
        lane_id = lax.broadcasted_iota(jnp.int32, (cz, slots), 0)
        for o in range(n_brk):
            cell = targets_ref[o : o + 1]
            row = jnp.where(cell < 0, -1, cell // cz - top)
            part = slice(o * slots, (o + 1) * slots)
            rows_ref[:, part] = jnp.where(row_id == row, 1.0, 0.0).astype(jnp.bfloat16)
            lanes_ref[:, part] = jnp.where(lane_id == cell % cz, 1.0, 0.0).astype(jnp.bfloat16)
        return lax.dot_general(
            rows_ref[...], lanes_ref[...], NT, preferred_element_type=jnp.float32
        )

    covered = mark(cell_out, 0, cx * cy, rows_hot, lanes_hot)

    block_id = lax.broadcasted_iota(jnp.int32, (4 * nblk, slots), 0) % nblk

    def interpolated(r):
        asked = req_in[r]
        wanted = asked[0:1].astype(jnp.int32)
        low = asked[1:2].astype(jnp.int32)
        hot = jnp.where(block_id == wanted, 1.0, 0.0).astype(jnp.bfloat16)
        picked = jnp.dot(turned[...], hot, preferred_element_type=jnp.float32)
        fx = factors(low // 32, asked[2:3], 4)
        fy = factors((low // 8) % 4, asked[3:4], 4)
        z_id = lax.broadcasted_iota(jnp.int32, (8, slots), 0)
        low_z = low % 8
        wz = asked[4:5]
        fz = jnp.where(z_id == low_z, 1.0 - wz, jnp.where(z_id == low_z + 1, wz, 0.0))
        tables = [fx[i] * fy[j] * fz for i in range(4) for j in range(4)]
        sums = []
        for v in range(nvars):
            total = None
            for i, table in enumerate(tables):
                start = v * block + 8 * i
                term = picked[start : start + 8] * table
                total = term if total is None else total + term
            sums.append(jnp.sum(total, axis=0, keepdims=True))
        return jnp.concatenate(sums + [blank], axis=0)

    answers = []

    for k in range(n_brk):
        if k > 0:
            asks[k - 1].wait_recv()
        r = lax.rem(b + n_brk - k, n_brk)
        res[r + 1] = interpolated(r)
    res[0] = res[n_brk]
    res[n_brk + 1] = res[1]
    for k in range(1, n_brk):
        o = lax.rem(b + k, n_brk)
        answers.append(
            send(res.at[pl.ds(o, 3)], val_in.at[b], sems, value_base + k, (g, o))
        )
    for v in range(2, nvars):
        send_raw(v)
    for slot in range(3):
        val_in[b, slot] = res[b + slot]
    covered_side = []
    for side, top in ((0, (cx - 3) * cy), (1, 0)):
        targets[side].wait_recv()
        covered_side.append(
            mark(cell_in.at[side], top, 3 * cy, rows_side.at[side], lanes_side.at[side])
        )
    for pending in answers:
        pending.wait_recv()

    def placed(slot, v, rows, lanes):
        row = jnp.concatenate([val_in[o, slot, v : v + 1] for o in range(n_brk)], axis=1)
        high = row.astype(jnp.bfloat16)
        rest = (row - high.astype(jnp.float32)).astype(jnp.bfloat16)
        spread = jnp.concatenate([lanes * high, lanes * rest], axis=0)
        both = lax.dot_general(rows, spread, NT, preferred_element_type=jnp.float32)
        return both[:, :cz] + both[:, cz:]

    for v in range(nvars):
        landed = placed(1, v, rows_hot[...], lanes_hot[...])
        for x in range(cx):
            part = slice(x * cy, (x + 1) * cy)
            plane = jnp.where(covered[part] > 0.5, landed[part], field[v, x])
            u0[v, 3 + x] = plane
            y0[v, x, 8 : 8 + cy] = plane

    def send_y(stage, y):
        for v in range(nvars):
            for k in range(3):
                ysend[stage, 0, k, v] = y[v, :, 8 + cy - 3 + k, :]
                ysend[stage, 1, k, v] = y[v, :, 8 + k, :]
        first = exchange_base + 4 * stage
        return [
            send(ysend.at[stage, 0], yrecv.at[stage, 0], sems, first, (up_g, b)),
            send(ysend.at[stage, 1], yrecv.at[stage, 1], sems, first + 1, (down_g, b)),
        ]

    def land_y(stage, y, pending):
        for copy in pending:
            copy.wait_recv()
        for v in range(nvars):
            for k in range(3):
                y[v, :, 5 + k, :] = yrecv[stage, 0, k, v]
                y[v, :, 8 + cy + k, :] = yrecv[stage, 1, k, v]
        copies.extend(pending)

    def section(u, y, store, start, stop):
        def plane(x, carry):
            centers = [u[v, x + 3] for v in range(nvars)]
            for v in range(nvars):
                total = coef[v, 3] * centers[v]
                for k in (0, 1, 2, 4, 5, 6):
                    total = total + coef[v, k] * u[v, x + k]
                    total = total + coef[v, 7 + k] * y[v, x, 5 + k : 5 + k + cy]
                    total = total + coef[v, 14 + k] * pltpu.roll(
                        centers[v], (3 - k) % cz, 1
                    )
                for w in range(nvars):
                    total = total + coef[v, 21 + w] * centers[w]
                store(x, v, centers[v] + total)
            return carry

        lax.fori_loop(start, stop, plane, 0)

    def store_first(x, v, value):
        u1[v, x + 3] = value
        y1[v, x, 8 : 8 + cy] = value

    def store_last(x, v, value):
        out[v, x] = 0.5 * u0[v, x + 3] + 0.5 * value

    y_pending = send_y(0, y0)
    for copy in raw:
        copy.wait_recv()
    for side, slot, start in ((0, 0, 0), (1, 2, cx + 3)):
        for v in range(nvars):
            landed = placed(slot, v, rows_side[side], lanes_side[side])
            for x in range(3):
                part = slice(x * cy, (x + 1) * cy)
                u0[v, start + x] = jnp.where(
                    covered_side[side][part] > 0.5, landed[part], u0[v, start + x]
                )
    land_y(0, y0, y_pending)

    section(u0, y0, store_first, 0, 3)
    section(u0, y0, store_first, cx - 3, cx)
    first = exchange_base + 2
    x_pending = [
        send(u1.at[:, pl.ds(cx, 3)], faces.at[0], sems, first, (g, up_b)),
        send(u1.at[:, pl.ds(3, 3)], faces.at[1], sems, first + 1, (g, down_b)),
    ]
    section(u0, y0, store_first, 3, cx - 3)
    y_pending = send_y(1, y1)
    zero = jnp.zeros((cy, cz), jnp.float32)
    for v in range(nvars):
        for x in range(3):
            u1[v, x] = zero
            u1[v, cx + 3 + x] = zero
    land_y(1, y1, y_pending)
    section(u1, y1, store_last, 0, cx)
    for copy in x_pending:
        copy.wait_recv()
    for v in range(nvars):
        for x in range(3):
            low = out[v, x]
            for k in range(3 - x):
                low = low + (0.5 * coef[v, k]) * faces[0, v, x + k]
            out[v, x] = low
            top = out[v, cx - 1 - x]
            for k in range(3 - x):
                top = top + (0.5 * coef[v, 6 - k]) * faces[1, v, 2 - x - k]
            out[v, cx - 1 - x] = top
    for copy in copies + asks + targets + raw + answers + x_pending:
        copy.wait_send()


def body(
    n_grp, n_brk, field, donors, donor_block, donor_corner, donor_weight, fringe_count,
    fringe_cell, velocity, mixing,
):
    nvars, cx, cy, cz = field.shape
    owners, slots = donor_block.shape[2:]
    vmem = pl.BlockSpec(memory_space=pltpu.VMEM)
    hbm = pl.BlockSpec(memory_space=pltpu.HBM)
    i32 = jnp.int32
    f32 = jnp.float32
    nsem = 4 * n_brk + 2 + 2 * nvars + 8
    return pl.pallas_call(
        functools.partial(kernel, n_grp, n_brk),
        out_shape=jax.ShapeDtypeStruct(field.shape, f32),
        in_specs=[hbm] * 9,
        out_specs=vmem,
        scratch_shapes=[
            pltpu.VMEM(field.shape, f32),
            pltpu.VMEM(donors.shape, f32),
            pltpu.VMEM((owners, slots), i32),
            pltpu.VMEM((owners, slots), i32),
            pltpu.VMEM((3, owners, slots), f32),
            pltpu.SMEM((owners,), i32),
            pltpu.VMEM((owners, slots), i32),
            pltpu.SMEM(velocity.shape, f32),
            pltpu.SMEM(mixing.shape, f32),
            pltpu.SemaphoreType.DMA((9,)),
            pltpu.VMEM((owners, 8, slots), f32),
            pltpu.VMEM((owners, 8, slots), f32),
            pltpu.VMEM((owners + 2, 8, slots), f32),
            pltpu.VMEM((owners, 3, 8, slots), f32),
            pltpu.VMEM((owners, slots), jnp.int32),
            pltpu.VMEM((2, owners, slots), jnp.int32),
            pltpu.VMEM((donors.shape[1], 4 * donors.shape[0]), jnp.bfloat16),
            pltpu.VMEM((cx * cy, owners * slots), jnp.bfloat16),
            pltpu.VMEM((cz, owners * slots), jnp.bfloat16),
            pltpu.VMEM((2, 3 * cy, owners * slots), jnp.bfloat16),
            pltpu.VMEM((2, cz, owners * slots), jnp.bfloat16),
            pltpu.VMEM((nvars, cx + 6, cy, cz), f32),
            pltpu.VMEM((nvars, cx, cy + 16, cz), f32),
            pltpu.VMEM((nvars, cx + 6, cy, cz), f32),
            pltpu.VMEM((nvars, cx, cy + 16, cz), f32),
            pltpu.VMEM((2, nvars, 3, cy, cz), f32),
            pltpu.VMEM((2, 2, 3, nvars, cx, cz), f32),
            pltpu.VMEM((2, 2, 3, nvars, cx, cz), f32),
            pltpu.SMEM((nvars, 21 + nvars), f32),
            pltpu.SemaphoreType.DMA((nsem,)),
            pltpu.SemaphoreType.DMA((nsem,)),
        ],
        compiler_params=pltpu.CompilerParams(
            collective_id=0, has_side_effects=True, vmem_limit_bytes=32 << 20
        ),
    )(
        *[
            pltpu.with_memory_space_constraint(x, pltpu.HBM)
            for x in (
                field, donors, donor_block.reshape(owners, slots),
                donor_corner.reshape(owners, slots), donor_weight.reshape(3, owners, slots),
                fringe_count.reshape(owners), fringe_cell.reshape(owners, slots), velocity,
                mixing,
            )
        ]
    )


def solution(mesh):
    placed = (
        P(None, "brk", "grp", None),
        P(("grp", "brk"), None),
        P("grp", "brk", None, None),
        P("grp", "brk", None, None),
        P(None, "grp", "brk", None, None),
        P("grp", "brk", None),
        P("grp", "brk", None, None),
        P(),
        P(),
    )
    return jax.shard_map(
        functools.partial(body, mesh.shape["grp"], mesh.shape["brk"]),
        mesh=mesh, in_specs=placed, out_specs=P(None, "brk", "grp", None), check_vma=False,
    )
```

```python
import functools

import jax
import jax.numpy as jnp
from jax import lax
from jax.experimental import pallas as pl
from jax.experimental.pallas import tpu as pltpu
from jax.sharding import PartitionSpec as P

time_step = 0.3
PLUS = (-2.0 / 60, 15.0 / 60, -60.0 / 60, 20.0 / 60, 30.0 / 60, -3.0 / 60, 0.0)
MINUS = (0.0, 3.0 / 60, -30.0 / 60, -20.0 / 60, 60.0 / 60, -15.0 / 60, 2.0 / 60)
NT = (((1,), (1,)), ((), ()))
REACH = 3
DEEP = 2 * REACH
EDGE = 8
PAD = 2 * EDGE


def factors(low, weight, count):
    return [
        jnp.where(low == c, 1.0 - weight, jnp.where(low == c - 1, weight, 0.0))
        for c in range(count)
    ]


def kernel(
    n_grp, n_brk, field_in, donors_in, blk_in, corner_in, weight_in, counts_in, cells_in,
    velocity_in, mixing_in, out, field, donors, blk, corner, weight, counts, cells, velocity,
    mixing, req, req_in, res, val_in, cell_out, cell_in, turned, rows_hot, lanes_hot, rows_side,
    lanes_side, u, first, relay, coef, in_sems, send_sems, recv_sems,
):
    nvars, cx, cy, cz = field_in.shape
    nblk = donors.shape[0]
    block = donors.shape[1] // nvars
    slots = cz
    g = lax.axis_index("grp")
    b = lax.axis_index("brk")
    odd = lax.rem(b, 2)
    partner = b + 1 - 2 * odd
    other = lax.rem(b + n_brk - 1 + 2 * odd, n_brk)
    onward = lax.rem(b + n_brk + 2 - 4 * odd, n_brk)
    up_g, down_g = lax.rem(g + 1, n_grp), lax.rem(g + n_grp - 1, n_grp)
    own = pl.ds(PAD, cy)

    def natural(p):
        return p + odd * (cx - 1 - 2 * p)

    loads = [
        pltpu.make_async_copy(src, dst, in_sems.at[i])
        for i, (src, dst) in enumerate(
            [
                (blk_in, blk), (corner_in, corner), (weight_in, weight), (counts_in, counts),
                (cells_in, cells), (velocity_in, velocity), (mixing_in, mixing),
                (donors_in, donors),
            ]
            + [(field_in.at[:, natural(p)], field.at[p]) for p in range(cx)]
        )
    ]
    for load in loads:
        load.start()

    barrier = pltpu.get_barrier_semaphore()
    for k in range(1, n_brk):
        pl.semaphore_signal(
            barrier, inc=1, device_id=(g, lax.rem(b + k, n_brk)),
            device_id_type=pl.DeviceIdType.MESH,
        )
    for where in (up_g, down_g):
        pl.semaphore_signal(
            barrier, inc=1, device_id=(where, b), device_id_type=pl.DeviceIdType.MESH
        )

    index = [0]
    started = []

    def send(src, dst, where):
        i = index[0]
        index[0] = i + 1
        copy = pltpu.make_async_remote_copy(
            src_ref=src, dst_ref=dst, send_sem=send_sems.at[i], recv_sem=recv_sems.at[i],
            device_id=where, device_id_type=pl.DeviceIdType.MESH,
        )
        copy.start()
        started.append(copy)
        return copy

    for load in loads[:8]:
        load.wait()
    blank = jnp.zeros((3, slots), jnp.float32)
    for o in range(n_brk):
        req[o] = jnp.concatenate(
            [
                blk[o : o + 1].astype(jnp.float32),
                corner[o : o + 1].astype(jnp.float32),
                weight[0, o : o + 1],
                weight[1, o : o + 1],
                weight[2, o : o + 1],
                blank,
            ],
            axis=0,
        )
    req_in[b] = req[b]
    slot_id = lax.broadcasted_iota(jnp.int32, (1, slots), 1)
    for o in range(n_brk):
        cell_out[o : o + 1] = jnp.where(slot_id < counts[o], cells[o : o + 1], -1)
    for v in range(nvars):
        center = 0.0
        for d in range(3):
            speed = velocity[d, v]
            fast = jnp.maximum(speed, 0.0) * (-time_step)
            slow = jnp.minimum(speed, 0.0) * (-time_step)
            for k in range(7):
                value = fast * PLUS[k] + slow * MINUS[k]
                if d == 0:
                    value = jnp.where(odd == 1, fast * PLUS[6 - k] + slow * MINUS[6 - k], value)
                if k == 3:
                    center = center + value
                else:
                    coef[v, d * 7 + k] = value
        coef[v, 3] = center
        for w in range(nvars):
            coef[v, 21 + w] = mixing[v, w] * (-time_step)
    for load in loads[8:]:
        load.wait()
    pl.semaphore_wait(barrier, n_brk + 1)

    asks = []
    for k in range(1, n_brk):
        o = lax.rem(b + k, n_brk)
        asks.append(send(req.at[o], req_in.at[b], (g, o)))
    cells_sent = [
        send(cell_out, cell_in.at[0], (g, other)), send(cell_out, cell_in.at[1], (g, partner))
    ]
    mirror = DEEP + 2 * cx - 1
    direct = {}

    def give(p, blended):
        src = u.at[DEEP + p, :, own] if blended else field.at[p]
        dst = u.at[mirror - p, :, own] if p >= cx - DEEP else relay.at[p]
        direct[p] = send(src, dst, (g, partner))

    passed = {}

    def pass_on(p):
        direct[p].wait_recv()
        src = u.at[mirror - p, :, own] if p >= cx - DEEP else relay.at[p]
        passed[p] = send(src, u.at[DEEP - 1 - p, :, own], (g, onward))

    give(0, False)
    give(1, False)

    whole = donors[...]
    one = whole.astype(jnp.bfloat16).astype(jnp.float32)
    two = (whole - one).astype(jnp.bfloat16).astype(jnp.float32)
    three = whole - one - two
    stacked = jnp.concatenate([one, two, three, jnp.zeros_like(whole)], axis=0)
    turned[...] = jnp.transpose(stacked).astype(jnp.bfloat16)

    def mark(targets_ref, flip, top, height, rows_ref, lanes_ref):
        row_id = lax.broadcasted_iota(jnp.int32, (height, slots), 0)
        lane_id = lax.broadcasted_iota(jnp.int32, (cz, slots), 0)
        for o in range(n_brk):
            cell = targets_ref[o : o + 1]
            row = cell // cz
            x = row // cy
            row = row + (flip * (cx - 1 - 2 * x) - top) * cy
            row = jnp.where(cell < 0, -1, row)
            part = slice(o * slots, (o + 1) * slots)
            rows_ref[:, part] = jnp.where(row_id == row, 1.0, 0.0).astype(jnp.bfloat16)
            lanes_ref[:, part] = jnp.where(lane_id == cell % cz, 1.0, 0.0).astype(jnp.bfloat16)
        return lax.dot_general(
            rows_ref[...], lanes_ref[...], NT, preferred_element_type=jnp.float32
        )

    covered = mark(cell_out, odd, 0, cx * cy, rows_hot, lanes_hot)

    block_id = lax.broadcasted_iota(jnp.int32, (4 * nblk, slots), 0) % nblk

    def interpolated(r):
        asked = req_in[r]
        wanted = asked[0:1].astype(jnp.int32)
        low = asked[1:2].astype(jnp.int32)
        hot = jnp.where(block_id == wanted, 1.0, 0.0).astype(jnp.bfloat16)
        picked = jnp.dot(turned[...], hot, preferred_element_type=jnp.float32)
        fx = factors(low // 32, asked[2:3], 4)
        fy = factors((low // 8) % 4, asked[3:4], 4)
        z_id = lax.broadcasted_iota(jnp.int32, (8, slots), 0)
        low_z = low % 8
        wz = asked[4:5]
        fz = jnp.where(z_id == low_z, 1.0 - wz, jnp.where(z_id == low_z + 1, wz, 0.0))
        tables = [fx[i] * fy[j] * fz for i in range(4) for j in range(4)]
        sums = []
        for v in range(nvars):
            total = None
            for i, table in enumerate(tables):
                start = v * block + 8 * i
                term = picked[start : start + 8] * table
                total = term if total is None else total + term
            sums.append(jnp.sum(total, axis=0, keepdims=True))
        return jnp.concatenate(sums + [blank], axis=0)

    for k in range(n_brk):
        if k > 0:
            asks[k - 1].wait_recv()
        r = lax.rem(b + n_brk - k, n_brk)
        res[r + 1] = interpolated(r)
    res[0] = res[n_brk]
    res[n_brk + 1] = res[1]
    answers = []
    for k in range(1, n_brk):
        o = lax.rem(b + k, n_brk)
        answers.append(send(res.at[pl.ds(o, 3)], val_in.at[b], (g, o)))
    give(cx - 1, False)
    give(cx - 2, False)
    for slot in range(3):
        val_in[b, slot] = res[b + slot]

    covered_side = []
    for side, top in ((0, 0), (1, cx - 2)):
        cells_sent[side].wait_recv()
        covered_side.append(
            mark(cell_in.at[side], 1 - odd, top, 2 * cy, rows_side.at[side], lanes_side.at[side])
        )
    pass_on(0)
    pass_on(1)
    for pending in answers:
        pending.wait_recv()

    def placed(slot, v, rows, lanes):
        row = jnp.concatenate([val_in[o, slot, v : v + 1] for o in range(n_brk)], axis=1)
        high = row.astype(jnp.bfloat16)
        rest = (row - high.astype(jnp.float32)).astype(jnp.bfloat16)
        spread = jnp.concatenate([lanes * high, lanes * rest], axis=0)
        both = lax.dot_general(rows, spread, NT, preferred_element_type=jnp.float32)
        return both[:, :cz] + both[:, cz:]

    for v in range(nvars):
        landed = placed(1, v, rows_hot[...], lanes_hot[...])
        for p in range(cx):
            part = slice(p * cy, (p + 1) * cy)
            u[DEEP + p, v, PAD : PAD + cy] = jnp.where(
                covered[part] > 0.5, landed[part], field[p, v]
            )
    for p in (2, 5, 3, 4):
        give(p, True)

    def edges(positions):
        return [
            send(
                u.at[positions, :, pl.ds(PAD + cy - EDGE, EDGE)],
                u.at[positions, :, pl.ds(PAD - EDGE, EDGE)], (up_g, b),
            ),
            send(
                u.at[positions, :, pl.ds(PAD, EDGE)],
                u.at[positions, :, pl.ds(PAD + cy, EDGE)], (down_g, b),
            ),
        ]

    def wait_all(copies):
        for copy in copies:
            copy.wait_recv()

    own_edges = edges(pl.ds(DEEP, cx))

    for side, slot, positions, arrivals in (
        (1, 2 - 2 * odd, (DEEP + cx + 1, DEEP + cx), (direct, (cx - 1, cx - 2))),
        (0, 2 * odd, (DEEP - 1, DEEP - 2), (passed, (0, 1))),
    ):
        for p in arrivals[1]:
            arrivals[0][p].wait_recv()
        for v in range(nvars):
            landed = placed(slot, v, rows_side[side], lanes_side[side])
            for i, q in enumerate(positions):
                part = slice(i * cy, (i + 1) * cy)
                u[q, v, PAD : PAD + cy] = jnp.where(
                    covered_side[side][part] > 0.5, landed[part], u[q, v, PAD : PAD + cy]
                )
    near_edges = edges(pl.ds(DEEP + cx, 2)) + edges(pl.ds(DEEP - 2, 2))

    def section(src, shift, low, height, store, start, stop):
        def plane(q, carry):
            centers = [src[q, v, low : low + height] for v in range(nvars)]
            for v in range(nvars):
                total = coef[v, 3] * centers[v]
                for k in (0, 1, 2, 4, 5, 6):
                    total = total + coef[v, k] * src[q + (k - 3), v, low : low + height]
                    total = total + coef[v, 7 + k] * src[
                        q, v, low + k - 3 : low + k - 3 + height
                    ]
                    total = total + coef[v, 14 + k] * pltpu.roll(
                        centers[v], (3 - k) % cz, 1
                    )
                for w in range(nvars):
                    total = total + coef[v, 21 + w] * centers[w]
                store(q, v, centers[v] + total)
            return carry

        lax.fori_loop(start + shift, stop + shift, plane, 0)

    def inner(start, stop):
        def store(q, v, value):
            first[q - REACH, v, PAD - EDGE : PAD + cy + EDGE] = value

        section(u, DEEP, PAD - EDGE, cy + 2 * EDGE, store, start, stop)

    def outer(start, stop):
        def store(q, v, value):
            first[q - REACH, v, PAD : PAD + cy] = value

        section(u, DEEP, PAD, cy, store, start, stop)

    def final(start, stop):
        def store(q, v, value):
            out[v, natural(q - REACH)] = (
                0.5 * u[q + REACH, v, PAD : PAD + cy] + 0.5 * value
            )

        section(first, REACH, PAD, cy, store, start, stop)

    pass_on(2)
    wait_all(own_edges)
    inner(3, cx - 3)
    pass_on(5)
    upper_edges = edges(pl.ds(DEEP + cx + 2, 1))
    wait_all(near_edges)
    inner(1, 3)
    inner(cx - 3, cx - 1)
    pass_on(3)
    passed[2].wait_recv()
    lower_edges = edges(pl.ds(DEEP - 3, 1))
    pass_on(4)
    wait_all(upper_edges)
    inner(cx - 1, cx)
    outer(cx, cx + 3)
    final(cx - 4, cx)
    wait_all(lower_edges)
    inner(0, 1)
    final(3, cx - 4)
    passed[5].wait_recv()
    passed[3].wait_recv()
    outer(-1, 0)
    final(2, 3)
    passed[4].wait_recv()
    outer(-3, -1)
    final(0, 2)
    for copy in started:
        copy.wait_send()


def body(
    n_grp, n_brk, field, donors, donor_block, donor_corner, donor_weight, fringe_count,
    fringe_cell, velocity, mixing,
):
    nvars, cx, cy, cz = field.shape
    owners, slots = donor_block.shape[2:]
    hbm = pl.BlockSpec(memory_space=pltpu.HBM)
    f32 = jnp.float32
    i32 = jnp.int32
    nsem = 2 * n_brk + 28
    rows = cy + 2 * PAD
    return pl.pallas_call(
        functools.partial(kernel, n_grp, n_brk),
        out_shape=jax.ShapeDtypeStruct(field.shape, f32),
        in_specs=[hbm] * 9,
        out_specs=pl.BlockSpec(memory_space=pltpu.VMEM),
        scratch_shapes=[
            pltpu.VMEM((cx, nvars, cy, cz), f32),
            pltpu.VMEM(donors.shape, f32),
            pltpu.VMEM((owners, slots), i32),
            pltpu.VMEM((owners, slots), i32),
            pltpu.VMEM((3, owners, slots), f32),
            pltpu.SMEM((owners,), i32),
            pltpu.VMEM((owners, slots), i32),
            pltpu.SMEM(velocity.shape, f32),
            pltpu.SMEM(mixing.shape, f32),
            pltpu.VMEM((owners, 8, slots), f32),
            pltpu.VMEM((owners, 8, slots), f32),
            pltpu.VMEM((owners + 2, 8, slots), f32),
            pltpu.VMEM((owners, 3, 8, slots), f32),
            pltpu.VMEM((owners, slots), i32),
            pltpu.VMEM((2, owners, slots), i32),
            pltpu.VMEM((donors.shape[1], 4 * donors.shape[0]), jnp.bfloat16),
            pltpu.VMEM((cx * cy, owners * slots), jnp.bfloat16),
            pltpu.VMEM((cz, owners * slots), jnp.bfloat16),
            pltpu.VMEM((2, 2 * cy, owners * slots), jnp.bfloat16),
            pltpu.VMEM((2, cz, owners * slots), jnp.bfloat16),
            pltpu.VMEM((cx + 2 * DEEP, nvars, rows, cz), f32),
            pltpu.VMEM((cx + 2 * REACH, nvars, rows, cz), f32),
            pltpu.VMEM((2, nvars, cy, cz), f32),
            pltpu.SMEM((nvars, 21 + nvars), f32),
            pltpu.SemaphoreType.DMA((8 + cx,)),
            pltpu.SemaphoreType.DMA((nsem,)),
            pltpu.SemaphoreType.DMA((nsem,)),
        ],
        compiler_params=pltpu.CompilerParams(
            collective_id=0, has_side_effects=True, vmem_limit_bytes=32 << 20
        ),
    )(
        *[
            pltpu.with_memory_space_constraint(x, pltpu.HBM)
            for x in (
                field, donors, donor_block.reshape(owners, slots),
                donor_corner.reshape(owners, slots), donor_weight.reshape(3, owners, slots),
                fringe_count.reshape(owners), fringe_cell.reshape(owners, slots), velocity,
                mixing,
            )
        ]
    )


def solution(mesh):
    placed = (
        P(None, "brk", "grp", None),
        P(("grp", "brk"), None),
        P("grp", "brk", None, None),
        P("grp", "brk", None, None),
        P(None, "grp", "brk", None, None),
        P("grp", "brk", None),
        P("grp", "brk", None, None),
        P(),
        P(),
    )
    return jax.shard_map(
        functools.partial(body, mesh.shape["grp"], mesh.shape["brk"]),
        mesh=mesh, in_specs=placed, out_specs=P(None, "brk", "grp", None), check_vma=False,
    )
```

```python
import functools

import jax
import jax.numpy as jnp
from jax import lax
from jax.experimental import pallas as pl
from jax.experimental.pallas import tpu as pltpu
from jax.sharding import PartitionSpec as P

time_step = 0.3
PLUS = (-2.0 / 60, 15.0 / 60, -60.0 / 60, 20.0 / 60, 30.0 / 60, -3.0 / 60, 0.0)
MINUS = (0.0, 3.0 / 60, -30.0 / 60, -20.0 / 60, 60.0 / 60, -15.0 / 60, 2.0 / 60)
NT = (((1,), (1,)), ((), ()))
REACH = 3
DEEP = 2 * REACH
EDGE = 8
PAD = 2 * EDGE


def factors(low, weight, count):
    return [
        jnp.where(low == c, 1.0 - weight, jnp.where(low == c - 1, weight, 0.0))
        for c in range(count)
    ]


def kernel(
    n_grp, n_brk, field_in, donors_in, blk_in, corner_in, weight_in, counts_in, cells_in,
    velocity_in, mixing_in, out, field, donors, blk, corner, weight, counts, cells, velocity,
    mixing, req, req_in, res, val_in, cell_out, cell_in, turned, rows_hot, lanes_hot, rows_far,
    rows_near, lanes_side, landed_far, landed_near, u, first, blend, near, far, own_out, own_in,
    upper_out, upper_in, lower_out, lower_in, coef, in_sems, send_sems, recv_sems,
):
    nvars, cx, cy, cz = field_in.shape
    nblk = donors.shape[0]
    block = donors.shape[1] // nvars
    slots = cz
    g = lax.axis_index("grp")
    b = lax.axis_index("brk")
    odd = lax.rem(b, 2)
    partner = b + 1 - 2 * odd
    other = lax.rem(b + n_brk - 1 + 2 * odd, n_brk)
    onward = lax.rem(b + n_brk + 2 - 4 * odd, n_brk)
    up_g, down_g = lax.rem(g + 1, n_grp), lax.rem(g + n_grp - 1, n_grp)

    def natural(p):
        return p + odd * (cx - 1 - 2 * p)

    loads = [
        pltpu.make_async_copy(src, dst, in_sems.at[i])
        for i, (src, dst) in enumerate(
            [(blk_in, blk), (corner_in, corner), (weight_in, weight)]
            + [(field_in.at[:, natural(p)], field.at[p]) for p in (0, 1)]
            + [
                (donors_in, donors), (counts_in, counts), (cells_in, cells),
                (velocity_in, velocity), (mixing_in, mixing),
            ]
            + [(field_in.at[:, natural(p)], field.at[p]) for p in range(2, cx)]
        )
    ]
    for load in loads:
        load.start()

    barrier = pltpu.get_barrier_semaphore()
    for k in range(1, n_brk):
        pl.semaphore_signal(
            barrier, inc=1, device_id=(g, lax.rem(b + k, n_brk)),
            device_id_type=pl.DeviceIdType.MESH,
        )
    for where in (up_g, down_g):
        pl.semaphore_signal(
            barrier, inc=1, device_id=(where, b), device_id_type=pl.DeviceIdType.MESH
        )

    own_pack, upper_pack, lower_pack = (
        (own_out, own_in), (upper_out, upper_in), (lower_out, lower_in)
    )
    index = [0]
    started = []

    def send(src, dst, where):
        i = index[0]
        index[0] = i + 1
        copy = pltpu.make_async_remote_copy(
            src_ref=src, dst_ref=dst, send_sem=send_sems.at[i], recv_sem=recv_sems.at[i],
            device_id=where, device_id_type=pl.DeviceIdType.MESH,
        )
        copy.start()
        started.append(copy)
        return copy

    for load in loads[:3]:
        load.wait()
    for o in range(n_brk):
        req[o, 0] = blk[o : o + 1].astype(jnp.float32)
        req[o, 1] = corner[o : o + 1].astype(jnp.float32)
        for d in range(3):
            req[o, 2 + d] = weight[d, o : o + 1]
    for load in loads[3:5]:
        load.wait()
    pl.semaphore_wait(barrier, n_brk + 1)

    asks = []
    for k in range(1, n_brk):
        o = lax.rem(b + k, n_brk)
        asks.append(send(req.at[o], req_in.at[b], (g, o)))
    mirror = DEEP + 2 * cx - 1
    direct = {}

    def give(src, p, low=0, high=nvars):
        part = pl.ds(low, high - low)
        direct.setdefault(p, []).append(
            send(src.at[p, part], near.at[p, part], (g, partner))
        )

    passed = {}

    def wait_all(copies):
        for copy in copies:
            copy.wait_recv()

    def pass_on(p):
        wait_all(direct[p])
        passed[p] = send(near.at[p], far.at[p], (g, onward))

    def keep(p, low, high):
        for v in range(nvars):
            u[mirror - p, v, PAD + low : PAD + high] = near[p, v, low:high]

    def take(p):
        passed[p].wait_recv()
        for v in range(nvars):
            u[DEEP - 1 - p, v, PAD : PAD + cy] = far[p, v]

    give(field, 0)
    give(field, 1)
    for load in loads[5:]:
        load.wait()
    req_in[b] = req[b]
    slot_id = lax.broadcasted_iota(jnp.int32, (1, slots), 1)
    for o in range(n_brk):
        cell_out[o : o + 1] = jnp.where(slot_id < counts[o], cells[o : o + 1], -1)
    for v in range(nvars):
        center = 0.0
        for d in range(3):
            speed = velocity[d, v]
            fast = jnp.maximum(speed, 0.0) * (-time_step)
            slow = jnp.minimum(speed, 0.0) * (-time_step)
            for k in range(7):
                value = fast * PLUS[k] + slow * MINUS[k]
                if d == 0:
                    value = jnp.where(odd == 1, fast * PLUS[6 - k] + slow * MINUS[6 - k], value)
                if k == 3:
                    center = center + value
                else:
                    coef[v, d * 7 + k] = value
        coef[v, 3] = 1.0 + center + mixing[v, v] * (-time_step)
        for w in range(nvars):
            coef[v, 21 + w] = mixing[v, w] * (-time_step)
    cells_sent = [
        send(cell_out, cell_in.at[0], (g, other)), send(cell_out, cell_in.at[1], (g, partner))
    ]

    whole = donors[...]
    one = whole.astype(jnp.bfloat16).astype(jnp.float32)
    two = (whole - one).astype(jnp.bfloat16).astype(jnp.float32)
    three = whole - one - two
    stacked = jnp.concatenate([one, two, three, jnp.zeros_like(whole)], axis=0)
    turned[...] = jnp.transpose(stacked).astype(jnp.bfloat16)

    def mark(targets_ref, flip, planes, rows_ref, lanes_ref):
        row_id = lax.broadcasted_iota(jnp.int32, (len(planes) * cy, slots), 0)
        label = row_id + planes[0] * cy
        for i in range(1, len(planes)):
            jump = planes[i] - planes[i - 1] - 1
            if jump:
                label = label + jnp.where(row_id >= i * cy, jump * cy, 0)
        lane_id = lax.broadcasted_iota(jnp.int32, (cz, slots), 0)
        for o in range(n_brk):
            cell = targets_ref[o : o + 1]
            row = cell // cz
            x = row // cy
            row = jnp.where(cell < 0, -1, row + flip * (cx - 1 - 2 * x) * cy)
            part = slice(o * slots, (o + 1) * slots)
            rows_ref[:, part] = jnp.where(label == row, 1.0, 0.0).astype(jnp.bfloat16)
            lanes_ref[:, part] = jnp.where(lane_id == cell % cz, 1.0, 0.0).astype(jnp.bfloat16)
        return lax.dot_general(
            rows_ref[...], lanes_ref[...], NT, preferred_element_type=jnp.float32
        )

    covered = mark(cell_out, odd, range(cx), rows_hot, lanes_hot)

    block_id = lax.broadcasted_iota(jnp.int32, (4 * nblk, slots), 0) % nblk

    def interpolated(r):
        asked = req_in[r]
        wanted = asked[0].astype(jnp.int32)
        low = asked[1].astype(jnp.int32)
        hot = jnp.where(block_id == wanted, 1.0, 0.0).astype(jnp.bfloat16)
        picked = jnp.dot(turned[...], hot, preferred_element_type=jnp.float32)
        fx = factors(low // 32, asked[2], 4)
        fy = factors((low // 8) % 4, asked[3], 4)
        z_id = lax.broadcasted_iota(jnp.int32, (8, slots), 0)
        low_z = low % 8
        wz = asked[4]
        fz = jnp.where(z_id == low_z, 1.0 - wz, jnp.where(z_id == low_z + 1, wz, 0.0))
        tables = [fx[i] * fy[j] * fz for i in range(4) for j in range(4)]
        sums = []
        for v in range(nvars):
            total = None
            for i, table in enumerate(tables):
                start = v * block + 8 * i
                term = picked[start : start + 8] * table
                total = term if total is None else total + term
            sums.append(jnp.sum(total, axis=0, keepdims=True))
        for v in range(nvars):
            res[r + 1, v] = sums[v]

    for k in range(n_brk):
        if k > 0:
            asks[k - 1].wait_recv()
        if k == n_brk // 2:
            give(field, 2, 0, 3)
        r = lax.rem(b + n_brk - k, n_brk)
        interpolated(r)
    res[0] = res[n_brk]
    res[n_brk + 1] = res[1]
    answers = []
    for k in range(1, n_brk):
        o = lax.rem(b + k, n_brk)
        answers.append(send(res.at[pl.ds(o, 3)], val_in.at[b], (g, o)))
    for slot in range(3):
        val_in[b, slot] = res[b + slot]

    raw_planes = ((0, 1, 2, 3, 5), (2, 3, 5))
    rows_of = (rows_far, rows_near)
    covered_side = []
    for side in range(2):
        cells_sent[side].wait_recv()
        covered_side.append(
            mark(
                cell_in.at[side], 1 - odd, raw_planes[side], rows_of[side], lanes_side.at[side]
            )
        )
    pass_on(0)
    give(field, 2, 3)
    give(field, 5)
    give(field, 3)
    pass_on(1)
    for pending in answers:
        pending.wait_recv()

    def placed(slot, v, rows, lanes):
        row = jnp.concatenate([val_in[o, slot, v] for o in range(n_brk)], axis=1)
        high = row.astype(jnp.bfloat16)
        rest = (row - high.astype(jnp.float32)).astype(jnp.bfloat16)
        spread = jnp.concatenate([lanes * high, lanes * rest], axis=0)
        both = lax.dot_general(rows, spread, NT, preferred_element_type=jnp.float32)
        return both[:, :cz] + both[:, cz:]

    for v in range(nvars):
        landed = placed(1, v, rows_hot[...], lanes_hot[...])
        for p in range(cx):
            part = slice(p * cy, (p + 1) * cy)
            plane = jnp.where(covered[part] > 0.5, landed[part], field[p, v])
            u[DEEP + p, v, PAD : PAD + cy] = plane
            if p in (4, cx - 2, cx - 1):
                blend[p, v] = plane
    faces = pl.ds(cx - 2, 2)

    def give_rows(low, height):
        part = (faces, slice(None), pl.ds(low, height))
        return send(blend.at[part], near.at[part], (g, partner))

    give(blend, 4)
    outer_rows = [give_rows(0, EDGE), give_rows(cy - EDGE, EDGE)]
    inner_rows = [give_rows(EDGE, cy - 2 * EDGE)]

    def edges(packs, q0):
        out_pack, in_pack = packs
        _, count, _, steps, step, _ = out_pack.shape
        for i in range(count):
            for v in range(nvars):
                for k in range(steps):
                    top = PAD + cy + (k - steps) * step
                    low = PAD + k * step
                    out_pack[0, i, v, k] = u[q0 + i, v, top : top + step]
                    out_pack[1, i, v, k] = u[q0 + i, v, low : low + step]
        return [
            send(out_pack.at[0], in_pack.at[0], (up_g, b)),
            send(out_pack.at[1], in_pack.at[1], (down_g, b)),
        ]

    def land(copies, packs, q0):
        wait_all(copies)
        in_pack = packs[1]
        _, count, _, steps, step, _ = in_pack.shape
        for i in range(count):
            for v in range(nvars):
                for k in range(steps):
                    low = PAD + (k - steps) * step
                    top = PAD + cy + k * step
                    u[q0 + i, v, low : low + step] = in_pack[0, i, v, k]
                    u[q0 + i, v, top : top + step] = in_pack[1, i, v, k]

    own_edges = edges(own_pack, DEEP)

    pass_on(2)
    landed_of = (landed_far, landed_near)
    for side, slot in ((1, 2 - 2 * odd), (0, 2 * odd)):
        for v in range(nvars):
            landed_of[side][v] = placed(slot, v, rows_of[side][...], lanes_side[side])

    def settle(side, raw, wanted):
        for p in wanted:
            i = raw_planes[side].index(p)
            q = mirror - p if side else DEEP - 1 - p
            part = slice(i * cy, (i + 1) * cy)
            for v in range(nvars):
                u[q, v, PAD : PAD + cy] = jnp.where(
                    covered_side[side][part] > 0.5, landed_of[side][v, part], raw[p, v]
                )

    def section(src, shift, low, height, store, start, stop):
        def group(first_q, count):
            for v in range(nvars):
                c = [coef[v, k] for k in range(21 + nvars)]
                for q in [first_q + n for n in range(count)]:
                    mid = src[q, v, low : low + height]
                    total = c[3] * mid
                    for k in (0, 1, 2, 4, 5, 6):
                        total = total + c[k] * src[q + (k - 3), v, low : low + height]
                        total = total + c[7 + k] * src[
                            q, v, low + k - 3 : low + k - 3 + height
                        ]
                        total = total + c[14 + k] * pltpu.roll(mid, (3 - k) % cz, 1)
                    for w in range(nvars):
                        if w != v:
                            total = total + c[21 + w] * src[q, w, low : low + height]
                    store(q, v, total)

        q = start + shift
        while q < stop + shift:
            count = min(3, stop + shift - q)
            group(q, count)
            q = q + count

    def inner(start, stop):
        def store(q, v, value):
            first[q - REACH, v, PAD - EDGE : PAD + cy + EDGE] = value

        section(u, DEEP, PAD - EDGE, cy + 2 * EDGE, store, start, stop)

    def outer(start, stop):
        def store(q, v, value):
            first[q - REACH, v, PAD : PAD + cy] = value

        section(u, DEEP, PAD, cy, store, start, stop)

    def final(start, stop):
        def store(q, v, value):
            out[v, natural(q - REACH)] = (
                0.5 * u[q + REACH, v, PAD : PAD + cy] + 0.5 * value
            )

        section(first, REACH, PAD, cy, store, start, stop)

    pass_on(5)
    pass_on(3)
    settle(1, near, (2, 3, 5))
    wait_all([passed[0], passed[1]])
    settle(0, far, (0, 1))
    wait_all([passed[2]])
    settle(0, far, (2,))
    lower_edges = edges(lower_pack, DEEP - REACH)
    land(own_edges, own_pack, DEEP)
    inner(3, cx - 3)
    wait_all(outer_rows)
    for p in (cx - 2, cx - 1):
        keep(p, 0, EDGE)
        keep(p, cy - EDGE, cy)
    upper_edges = edges(upper_pack, DEEP + cx)
    pass_on(4)
    keep(4, 0, cy)
    land(lower_edges, lower_pack, DEEP - REACH)
    inner(0, 3)
    wait_all([passed[5], passed[3]])
    settle(0, far, (5, 3))
    outer(-1, 0)
    land(upper_edges, upper_pack, DEEP + cx)
    wait_all(inner_rows)
    for p in (cx - 2, cx - 1):
        keep(p, EDGE, cy - EDGE)
    inner(cx - 3, cx)
    outer(cx, cx + 3)
    final(2, cx)
    early = len(started) - 2
    for copy in started[:early]:
        copy.wait_send()
    take(4)
    outer(-3, -1)
    final(0, 2)
    for copy in started[early:]:
        copy.wait_send()


def body(
    n_grp, n_brk, field, donors, donor_block, donor_corner, donor_weight, fringe_count,
    fringe_cell, velocity, mixing,
):
    nvars, cx, cy, cz = field.shape
    owners, slots = donor_block.shape[2:]
    hbm = pl.BlockSpec(memory_space=pltpu.HBM)
    f32 = jnp.float32
    i32 = jnp.int32
    nsem = 2 * n_brk + 29
    rows = cy + 2 * PAD
    field_brick = (cx, nvars, cy, cz)
    return pl.pallas_call(
        functools.partial(kernel, n_grp, n_brk),
        out_shape=jax.ShapeDtypeStruct(field.shape, f32),
        in_specs=[hbm] * 9,
        out_specs=pl.BlockSpec(memory_space=pltpu.VMEM),
        scratch_shapes=[
            pltpu.VMEM(field_brick, f32),
            pltpu.VMEM(donors.shape, f32),
            pltpu.VMEM((owners, slots), i32),
            pltpu.VMEM((owners, slots), i32),
            pltpu.VMEM((3, owners, slots), f32),
            pltpu.SMEM((owners,), i32),
            pltpu.VMEM((owners, slots), i32),
            pltpu.SMEM(velocity.shape, f32),
            pltpu.SMEM(mixing.shape, f32),
            pltpu.VMEM((owners, 5, 1, slots), f32),
            pltpu.VMEM((owners, 5, 1, slots), f32),
            pltpu.VMEM((owners + 2, nvars, 1, slots), f32),
            pltpu.VMEM((owners, 3, nvars, 1, slots), f32),
            pltpu.VMEM((owners, slots), i32),
            pltpu.VMEM((2, owners, slots), i32),
            pltpu.VMEM((donors.shape[1], 4 * donors.shape[0]), jnp.bfloat16),
            pltpu.VMEM((cx * cy, owners * slots), jnp.bfloat16),
            pltpu.VMEM((cz, owners * slots), jnp.bfloat16),
            pltpu.VMEM((5 * cy, owners * slots), jnp.bfloat16),
            pltpu.VMEM((3 * cy, owners * slots), jnp.bfloat16),
            pltpu.VMEM((2, cz, owners * slots), jnp.bfloat16),
            pltpu.VMEM((nvars, 5 * cy, cz), f32),
            pltpu.VMEM((nvars, 3 * cy, cz), f32),
            pltpu.VMEM((cx + 2 * DEEP, nvars, rows, cz), f32),
            pltpu.VMEM((cx + 2 * REACH, nvars, rows, cz), f32),
            pltpu.VMEM(field_brick, f32),
            pltpu.VMEM(field_brick, f32),
            pltpu.VMEM((DEEP, nvars, cy, cz), f32),
            pltpu.VMEM((2, cx, nvars, DEEP // 2, 2, cz), f32),
            pltpu.VMEM((2, cx, nvars, DEEP // 2, 2, cz), f32),
            pltpu.VMEM((2, REACH, nvars, REACH, 1, cz), f32),
            pltpu.VMEM((2, REACH, nvars, REACH, 1, cz), f32),
            pltpu.VMEM((2, REACH, nvars, REACH, 1, cz), f32),
            pltpu.VMEM((2, REACH, nvars, REACH, 1, cz), f32),
            pltpu.SMEM((nvars, 21 + nvars), f32),
            pltpu.SemaphoreType.DMA((8 + cx,)),
            pltpu.SemaphoreType.DMA((nsem,)),
            pltpu.SemaphoreType.DMA((nsem,)),
        ],
        compiler_params=pltpu.CompilerParams(
            collective_id=0, has_side_effects=True, vmem_limit_bytes=32 << 20
        ),
    )(
        *[
            pltpu.with_memory_space_constraint(x, pltpu.HBM)
            for x in (
                field, donors, donor_block.reshape(owners, slots),
                donor_corner.reshape(owners, slots), donor_weight.reshape(3, owners, slots),
                fringe_count.reshape(owners), fringe_cell.reshape(owners, slots), velocity,
                mixing,
            )
        ]
    )


def solution(mesh):
    placed = (
        P(None, "brk", "grp", None),
        P(("grp", "brk"), None),
        P("grp", "brk", None, None),
        P("grp", "brk", None, None),
        P(None, "grp", "brk", None, None),
        P("grp", "brk", None),
        P("grp", "brk", None, None),
        P(),
        P(),
    )
    return jax.shard_map(
        functools.partial(body, mesh.shape["grp"], mesh.shape["brk"]),
        mesh=mesh, in_specs=placed, out_specs=P(None, "brk", "grp", None), check_vma=False,
    )
```

```python
import functools

import jax
import jax.numpy as jnp
from jax import lax
from jax.experimental import pallas as pl
from jax.experimental.pallas import tpu as pltpu
from jax.sharding import PartitionSpec as P

time_step = 0.3
PLUS = (-2.0 / 60, 15.0 / 60, -60.0 / 60, 20.0 / 60, 30.0 / 60, -3.0 / 60, 0.0)
MINUS = (0.0, 3.0 / 60, -30.0 / 60, -20.0 / 60, 60.0 / 60, -15.0 / 60, 2.0 / 60)
NT = (((1,), (1,)), ((), ()))
REACH = 3
DEEP = 2 * REACH
EDGE = 8
PAD = 2 * EDGE


def factors(low, weight, count):
    return [
        jnp.where(low == c, 1.0 - weight, jnp.where(low == c - 1, weight, 0.0))
        for c in range(count)
    ]


def kernel(
    n_grp, n_brk, field_in, donors_in, blk_in, corner_in, weight_in, counts_in, cells_in,
    velocity_in, mixing_in, out, field, donors, blk, corner, weight, counts, cells, velocity,
    mixing, req, req_in, res, val_in, cell_out, cell_in, turned, rows_hot, lanes_hot, rows_far,
    rows_near, lanes_side, landed_far, landed_near, u, first, blend, near, far, own_out, own_in,
    upper_out, upper_in, lower_out, lower_in, coef, in_sems, send_sems, recv_sems,
):
    nvars, cx, cy, cz = field_in.shape
    nblk = donors.shape[0]
    block = donors.shape[1] // nvars
    slots = cz
    g = lax.axis_index("grp")
    b = lax.axis_index("brk")
    odd = lax.rem(b, 2)
    partner = b + 1 - 2 * odd
    other = lax.rem(b + n_brk - 1 + 2 * odd, n_brk)
    onward = lax.rem(b + n_brk + 2 - 4 * odd, n_brk)
    up_g, down_g = lax.rem(g + 1, n_grp), lax.rem(g + n_grp - 1, n_grp)

    def natural(p):
        return p + odd * (cx - 1 - 2 * p)

    loads = [
        pltpu.make_async_copy(src, dst, in_sems.at[i])
        for i, (src, dst) in enumerate(
            [(blk_in, blk), (corner_in, corner), (weight_in, weight)]
            + [(field_in.at[:, natural(p)], field.at[p]) for p in (0, 1)]
            + [
                (donors_in, donors), (counts_in, counts), (cells_in, cells),
                (velocity_in, velocity), (mixing_in, mixing),
            ]
            + [(field_in.at[:, natural(p)], field.at[p]) for p in range(2, cx)]
        )
    ]
    for load in loads:
        load.start()

    barrier = pltpu.get_barrier_semaphore()
    for k in range(1, n_brk):
        pl.semaphore_signal(
            barrier, inc=1, device_id=(g, lax.rem(b + k, n_brk)),
            device_id_type=pl.DeviceIdType.MESH,
        )
    for where in (up_g, down_g):
        pl.semaphore_signal(
            barrier, inc=1, device_id=(where, b), device_id_type=pl.DeviceIdType.MESH
        )

    own_pack, upper_pack, lower_pack = (
        (own_out, own_in), (upper_out, upper_in), (lower_out, lower_in)
    )
    index = [0]
    started = []

    def send(src, dst, where):
        i = index[0]
        index[0] = i + 1
        copy = pltpu.make_async_remote_copy(
            src_ref=src, dst_ref=dst, send_sem=send_sems.at[i], recv_sem=recv_sems.at[i],
            device_id=where, device_id_type=pl.DeviceIdType.MESH,
        )
        copy.start()
        started.append(copy)
        return copy

    for load in loads[:3]:
        load.wait()
    for o in range(n_brk):
        req[o, 0] = blk[o : o + 1].astype(jnp.float32)
        req[o, 1] = corner[o : o + 1].astype(jnp.float32)
        for d in range(3):
            req[o, 2 + d] = weight[d, o : o + 1]
    for load in loads[3:5]:
        load.wait()
    pl.semaphore_wait(barrier, n_brk + 1)

    asks = []
    for k in range(1, n_brk):
        o = lax.rem(b + k, n_brk)
        asks.append(send(req.at[o], req_in.at[b], (g, o)))
    mirror = DEEP + 2 * cx - 1
    direct = {}

    def give(src, p, low=0, high=nvars):
        part = pl.ds(low, high - low)
        direct.setdefault(p, []).append(
            send(src.at[p, part], near.at[p, part], (g, partner))
        )

    passed = {}

    def wait_all(copies):
        for copy in copies:
            copy.wait_recv()

    def pass_on(p):
        wait_all(direct[p])
        passed[p] = send(near.at[p], far.at[p], (g, onward))

    def keep(p, low, high):
        for v in range(nvars):
            u[mirror - p, v, PAD + low : PAD + high] = near[p, v, low:high]

    def take(p):
        passed[p].wait_recv()
        for v in range(nvars):
            u[DEEP - 1 - p, v, PAD : PAD + cy] = far[p, v]

    give(field, 0)
    give(field, 1)
    for load in loads[5:]:
        load.wait()
    req_in[b] = req[b]
    slot_id = lax.broadcasted_iota(jnp.int32, (1, slots), 1)
    for o in range(n_brk):
        cell_out[o : o + 1] = jnp.where(slot_id < counts[o], cells[o : o + 1], -1)
    for v in range(nvars):
        center = 0.0
        for d in range(3):
            speed = velocity[d, v]
            fast = jnp.maximum(speed, 0.0) * (-time_step)
            slow = jnp.minimum(speed, 0.0) * (-time_step)
            for k in range(7):
                value = fast * PLUS[k] + slow * MINUS[k]
                if d == 0:
                    value = jnp.where(odd == 1, fast * PLUS[6 - k] + slow * MINUS[6 - k], value)
                if k == 3:
                    center = center + value
                else:
                    coef[v, d * 7 + k] = value
        coef[v, 3] = 1.0 + center + mixing[v, v] * (-time_step)
        for w in range(nvars):
            coef[v, 21 + w] = mixing[v, w] * (-time_step)
    cells_sent = [
        send(cell_out, cell_in.at[0], (g, other)), send(cell_out, cell_in.at[1], (g, partner))
    ]

    whole = donors[...]
    one = whole.astype(jnp.bfloat16).astype(jnp.float32)
    two = (whole - one).astype(jnp.bfloat16).astype(jnp.float32)
    three = whole - one - two
    stacked = jnp.concatenate([one, two, three, jnp.zeros_like(whole)], axis=0)
    turned[...] = jnp.transpose(stacked).astype(jnp.bfloat16)

    def mark(targets_ref, flip, planes, rows_ref, lanes_ref):
        row_id = lax.broadcasted_iota(jnp.int32, (len(planes) * cy, slots), 0)
        label = row_id + planes[0] * cy
        for i in range(1, len(planes)):
            jump = planes[i] - planes[i - 1] - 1
            if jump:
                label = label + jnp.where(row_id >= i * cy, jump * cy, 0)
        lane_id = lax.broadcasted_iota(jnp.int32, (cz, slots), 0)
        for o in range(n_brk):
            cell = targets_ref[o : o + 1]
            row = cell // cz
            x = row // cy
            row = jnp.where(cell < 0, -1, row + flip * (cx - 1 - 2 * x) * cy)
            part = slice(o * slots, (o + 1) * slots)
            rows_ref[:, part] = jnp.where(label == row, 1.0, 0.0).astype(jnp.bfloat16)
            lanes_ref[:, part] = jnp.where(lane_id == cell % cz, 1.0, 0.0).astype(jnp.bfloat16)
        return lax.dot_general(
            rows_ref[...], lanes_ref[...], NT, preferred_element_type=jnp.float32
        )

    covered = mark(cell_out, odd, range(cx), rows_hot, lanes_hot)

    block_id = lax.broadcasted_iota(jnp.int32, (4 * nblk, slots), 0) % nblk

    def interpolated(r):
        asked = req_in[r]
        wanted = asked[0].astype(jnp.int32)
        low = asked[1].astype(jnp.int32)
        hot = jnp.where(block_id == wanted, 1.0, 0.0).astype(jnp.bfloat16)
        picked = jnp.dot(turned[...], hot, preferred_element_type=jnp.float32)
        fx = factors(low // 32, asked[2], 4)
        fy = factors((low // 8) % 4, asked[3], 4)
        z_id = lax.broadcasted_iota(jnp.int32, (8, slots), 0)
        low_z = low % 8
        wz = asked[4]
        fz = jnp.where(z_id == low_z, 1.0 - wz, jnp.where(z_id == low_z + 1, wz, 0.0))
        tables = [fx[i] * fy[j] * fz for i in range(4) for j in range(4)]
        sums = []
        for v in range(nvars):
            total = None
            for i, table in enumerate(tables):
                start = v * block + 8 * i
                term = picked[start : start + 8] * table
                total = term if total is None else total + term
            sums.append(jnp.sum(total, axis=0, keepdims=True))
        for v in range(nvars):
            res[r + 1, v] = sums[v]

    for k in range(n_brk):
        if k > 0:
            asks[k - 1].wait_recv()
        if k == n_brk // 2:
            give(field, 2)
        r = lax.rem(b + n_brk - k, n_brk)
        interpolated(r)
    res[0] = res[n_brk]
    res[n_brk + 1] = res[1]
    answers = []
    for k in range(1, n_brk):
        o = lax.rem(b + k, n_brk)
        answers.append(send(res.at[pl.ds(o, 3)], val_in.at[b], (g, o)))
    for slot in range(3):
        val_in[b, slot] = res[b + slot]

    raw_planes = ((0, 1, 2, 3, 5), (2, 3, 5))
    rows_of = (rows_far, rows_near)
    covered_side = []
    for side in range(2):
        cells_sent[side].wait_recv()
        covered_side.append(
            mark(
                cell_in.at[side], 1 - odd, raw_planes[side], rows_of[side], lanes_side.at[side]
            )
        )
    pass_on(0)
    give(field, 5)
    give(field, 3)
    pass_on(1)
    for pending in answers:
        pending.wait_recv()

    def placed(slot, v, rows, lanes):
        row = jnp.concatenate([val_in[o, slot, v] for o in range(n_brk)], axis=1)
        high = row.astype(jnp.bfloat16)
        rest = (row - high.astype(jnp.float32)).astype(jnp.bfloat16)
        spread = jnp.concatenate([lanes * high, lanes * rest], axis=0)
        both = lax.dot_general(rows, spread, NT, preferred_element_type=jnp.float32)
        return both[:, :cz] + both[:, cz:]

    for v in range(nvars):
        landed = placed(1, v, rows_hot[...], lanes_hot[...])
        for p in range(cx):
            part = slice(p * cy, (p + 1) * cy)
            plane = jnp.where(covered[part] > 0.5, landed[part], field[p, v])
            u[DEEP + p, v, PAD : PAD + cy] = plane
            if p in (4, cx - 2, cx - 1):
                blend[p, v] = plane
    faces = pl.ds(cx - 2, 2)

    def give_rows(low, height):
        part = (faces, slice(None), pl.ds(low, height))
        return send(blend.at[part], near.at[part], (g, partner))

    give(blend, 4)
    outer_rows = [give_rows(0, EDGE), give_rows(cy - EDGE, EDGE)]
    inner_rows = [give_rows(EDGE, cy - 2 * EDGE)]

    def edges(packs, q0):
        out_pack, in_pack = packs
        _, count, _, steps, step, _ = out_pack.shape
        for i in range(count):
            for v in range(nvars):
                for k in range(steps):
                    top = PAD + cy + (k - steps) * step
                    low = PAD + k * step
                    out_pack[0, i, v, k] = u[q0 + i, v, top : top + step]
                    out_pack[1, i, v, k] = u[q0 + i, v, low : low + step]
        return [
            send(out_pack.at[0], in_pack.at[0], (up_g, b)),
            send(out_pack.at[1], in_pack.at[1], (down_g, b)),
        ]

    def land(copies, packs, q0):
        wait_all(copies)
        in_pack = packs[1]
        _, count, _, steps, step, _ = in_pack.shape
        for i in range(count):
            for v in range(nvars):
                for k in range(steps):
                    low = PAD + (k - steps) * step
                    top = PAD + cy + k * step
                    u[q0 + i, v, low : low + step] = in_pack[0, i, v, k]
                    u[q0 + i, v, top : top + step] = in_pack[1, i, v, k]

    own_edges = edges(own_pack, DEEP)

    pass_on(2)
    landed_of = (landed_far, landed_near)
    for side, slot in ((1, 2 - 2 * odd), (0, 2 * odd)):
        for v in range(nvars):
            landed_of[side][v] = placed(slot, v, rows_of[side][...], lanes_side[side])

    def settle(side, raw, wanted):
        for p in wanted:
            i = raw_planes[side].index(p)
            q = mirror - p if side else DEEP - 1 - p
            part = slice(i * cy, (i + 1) * cy)
            for v in range(nvars):
                u[q, v, PAD : PAD + cy] = jnp.where(
                    covered_side[side][part] > 0.5, landed_of[side][v, part], raw[p, v]
                )

    def section(src, shift, low, height, store, start, stop):
        def group(first_q, count):
            for v in range(nvars):
                c = [coef[v, k] for k in range(21 + nvars)]
                for q in [first_q + n for n in range(count)]:
                    mid = src[q, v, low : low + height]
                    total = c[3] * mid
                    for k in (0, 1, 2, 4, 5, 6):
                        total = total + c[k] * src[q + (k - 3), v, low : low + height]
                        total = total + c[7 + k] * src[
                            q, v, low + k - 3 : low + k - 3 + height
                        ]
                        total = total + c[14 + k] * pltpu.roll(mid, (3 - k) % cz, 1)
                    for w in range(nvars):
                        if w != v:
                            total = total + c[21 + w] * src[q, w, low : low + height]
                    store(q, v, total)

        q = start + shift
        while q < stop + shift:
            count = min(3, stop + shift - q)
            group(q, count)
            q = q + count

    def inner(start, stop):
        def store(q, v, value):
            first[q - REACH, v, PAD - EDGE : PAD + cy + EDGE] = value

        section(u, DEEP, PAD - EDGE, cy + 2 * EDGE, store, start, stop)

    def outer(start, stop):
        def store(q, v, value):
            first[q - REACH, v, PAD : PAD + cy] = value

        section(u, DEEP, PAD, cy, store, start, stop)

    def final(start, stop):
        def store(q, v, value):
            out[v, natural(q - REACH)] = (
                0.5 * u[q + REACH, v, PAD : PAD + cy] + 0.5 * value
            )

        section(first, REACH, PAD, cy, store, start, stop)

    pass_on(5)
    pass_on(3)
    settle(1, near, (2, 3, 5))
    wait_all([passed[0], passed[1]])
    settle(0, far, (0, 1))
    wait_all([passed[2]])
    settle(0, far, (2,))
    lower_edges = edges(lower_pack, DEEP - REACH)
    land(own_edges, own_pack, DEEP)
    inner(3, cx - 3)
    wait_all(outer_rows)
    for p in (cx - 2, cx - 1):
        keep(p, 0, EDGE)
        keep(p, cy - EDGE, cy)
    upper_edges = edges(upper_pack, DEEP + cx)
    pass_on(4)
    keep(4, 0, cy)
    land(lower_edges, lower_pack, DEEP - REACH)
    inner(0, 3)
    wait_all([passed[5], passed[3]])
    settle(0, far, (5, 3))
    outer(-1, 0)
    land(upper_edges, upper_pack, DEEP + cx)
    wait_all(inner_rows)
    for p in (cx - 2, cx - 1):
        keep(p, EDGE, cy - EDGE)
    inner(cx - 3, cx)
    outer(cx, cx + 3)
    final(2, cx)
    early = len(started) - 2
    for copy in started[:early]:
        copy.wait_send()
    take(4)
    outer(-3, -1)
    final(0, 2)
    for copy in started[early:]:
        copy.wait_send()


def body(
    n_grp, n_brk, field, donors, donor_block, donor_corner, donor_weight, fringe_count,
    fringe_cell, velocity, mixing,
):
    nvars, cx, cy, cz = field.shape
    owners, slots = donor_block.shape[2:]
    hbm = pl.BlockSpec(memory_space=pltpu.HBM)
    f32 = jnp.float32
    i32 = jnp.int32
    nsem = 2 * n_brk + 29
    rows = cy + 2 * PAD
    field_brick = (cx, nvars, cy, cz)
    return pl.pallas_call(
        functools.partial(kernel, n_grp, n_brk),
        out_shape=jax.ShapeDtypeStruct(field.shape, f32),
        in_specs=[hbm] * 9,
        out_specs=pl.BlockSpec(memory_space=pltpu.VMEM),
        scratch_shapes=[
            pltpu.VMEM(field_brick, f32),
            pltpu.VMEM(donors.shape, f32),
            pltpu.VMEM((owners, slots), i32),
            pltpu.VMEM((owners, slots), i32),
            pltpu.VMEM((3, owners, slots), f32),
            pltpu.SMEM((owners,), i32),
            pltpu.VMEM((owners, slots), i32),
            pltpu.SMEM(velocity.shape, f32),
            pltpu.SMEM(mixing.shape, f32),
            pltpu.VMEM((owners, 5, 1, slots), f32),
            pltpu.VMEM((owners, 5, 1, slots), f32),
            pltpu.VMEM((owners + 2, nvars, 1, slots), f32),
            pltpu.VMEM((owners, 3, nvars, 1, slots), f32),
            pltpu.VMEM((owners, slots), i32),
            pltpu.VMEM((2, owners, slots), i32),
            pltpu.VMEM((donors.shape[1], 4 * donors.shape[0]), jnp.bfloat16),
            pltpu.VMEM((cx * cy, owners * slots), jnp.bfloat16),
            pltpu.VMEM((cz, owners * slots), jnp.bfloat16),
            pltpu.VMEM((5 * cy, owners * slots), jnp.bfloat16),
            pltpu.VMEM((3 * cy, owners * slots), jnp.bfloat16),
            pltpu.VMEM((2, cz, owners * slots), jnp.bfloat16),
            pltpu.VMEM((nvars, 5 * cy, cz), f32),
            pltpu.VMEM((nvars, 3 * cy, cz), f32),
            pltpu.VMEM((cx + 2 * DEEP, nvars, rows, cz), f32),
            pltpu.VMEM((cx + 2 * REACH, nvars, rows, cz), f32),
            pltpu.VMEM(field_brick, f32),
            pltpu.VMEM(field_brick, f32),
            pltpu.VMEM((DEEP, nvars, cy, cz), f32),
            pltpu.VMEM((2, cx, nvars, DEEP // 2, 2, cz), f32),
            pltpu.VMEM((2, cx, nvars, DEEP // 2, 2, cz), f32),
            pltpu.VMEM((2, REACH, nvars, REACH, 1, cz), f32),
            pltpu.VMEM((2, REACH, nvars, REACH, 1, cz), f32),
            pltpu.VMEM((2, REACH, nvars, REACH, 1, cz), f32),
            pltpu.VMEM((2, REACH, nvars, REACH, 1, cz), f32),
            pltpu.SMEM((nvars, 21 + nvars), f32),
            pltpu.SemaphoreType.DMA((8 + cx,)),
            pltpu.SemaphoreType.DMA((nsem,)),
            pltpu.SemaphoreType.DMA((nsem,)),
        ],
        compiler_params=pltpu.CompilerParams(
            collective_id=0, has_side_effects=True, vmem_limit_bytes=32 << 20
        ),
    )(
        *[
            pltpu.with_memory_space_constraint(x, pltpu.HBM)
            for x in (
                field, donors, donor_block.reshape(owners, slots),
                donor_corner.reshape(owners, slots), donor_weight.reshape(3, owners, slots),
                fringe_count.reshape(owners), fringe_cell.reshape(owners, slots), velocity,
                mixing,
            )
        ]
    )


def solution(mesh):
    placed = (
        P(None, "brk", "grp", None),
        P(("grp", "brk"), None),
        P("grp", "brk", None, None),
        P("grp", "brk", None, None),
        P(None, "grp", "brk", None, None),
        P("grp", "brk", None),
        P("grp", "brk", None, None),
        P(),
        P(),
    )
    return jax.shard_map(
        functools.partial(body, mesh.shape["grp"], mesh.shape["brk"]),
        mesh=mesh, in_specs=placed, out_specs=P(None, "brk", "grp", None), check_vma=False,
    )
```
